32 devices in a mesh: gx: 4 (over y, x), gy: 2 (over core), gz: 4 (over z).
Axes of the slice: x: 2, y: 2, z: 4, core: 2. Of those that a mesh axis runs over, the one named last changes fastest.
Arguments:
- rhs: float32 [3, 32, 32, 512], P(None, 'gx', 'gy', 'gz'), may hold values from -24 to 24
- conductivity: float32 [8], replicated, may hold values from 0.1 to 10
- fraction: float32 [3, 32, 32, 512], P(None, 'gx', 'gy', 'gz'), may hold values from 0.5 to 2
- region: int32 [32, 32, 512], P('gx', 'gy', 'gz'), may hold values from 0 to 7
- flags: int32 [3, 32, 32, 512], P(None, 'gx', 'gy', 'gz'), may hold values 0 or 1
Outputs:
- preconditioned: float32 [3, 32, 32, 512], P(None, 'gx', 'gy', 'gz')
The draws below stay inside these ranges and needn't reach their ends.
All inputs are finite; a program needn't handle non-finite values. No bound on the sum of `flags` on one device may be relied on, other than what follows from the above.
Results may differ from the reference program's by a relative error of at most 0.00002.
Values sent between devices are 32-bit elements; how exact they have to be, the bound alone decides.
A program may use at most 64 MiB of HBM per device.

```python
import math
import jax
import jax.numpy as jnp

REGIONS = 8
NX = 32
NY = 32
NZ = 512


def place_ends(values, stream_key, low, largest):
    shape = values.shape
    spot = [jax.random.randint(jax.random.fold_in(stream_key, axis), (), 0, shape[axis]) for axis in range(len(shape))]
    values = values.at[tuple(spot)].set(low)
    longest = shape.index(max(shape))
    spot[longest] = (spot[longest] + 1) % shape[longest]
    return values.at[tuple(spot)].set(largest)


def shard_levels(key, extent, split, low, high):
    def one(dim, blocks):
        heights = jax.random.uniform(jax.random.fold_in(jax.random.fold_in(key, 6), dim), (blocks,), jnp.float32, low / len(split), high / len(split))
        return jnp.repeat(jnp.exp(heights), extent[dim] // blocks).reshape((-1,) + (1,) * (len(extent) - dim - 1))

    loudness = one(*split[0])
    for cut in split[1:]:
        loudness = loudness * one(*cut)
    return loudness


def scatter_about(rng, dims, width, limit, shards=(), kind=jnp.bfloat16):
    loudness = shard_levels(rng, dims, shards, -0.22, 0.18) if shards else 1.0
    values = jax.random.normal(rng, dims, jnp.float32) * width * loudness
    return jnp.minimum(jnp.maximum(values, -limit), limit).astype(kind)


def setup_inputs(seed: int = 0) -> dict:
    arg_keys = jax.random.split(jax.random.key(seed), 6)
    rhs = scatter_about(arg_keys[0], (3, NX, NY, NZ), 4.0, 24.0, ((1, 4), (2, 2), (3, 4)), jnp.float32)
    conductivity = jnp.clip(jnp.exp(jax.random.uniform(arg_keys[1], (REGIONS,), jnp.float32, math.log(0.1), math.log(10.0))), 0.1, 10.0)
    fraction = jnp.clip(jnp.exp(math.log(2.0) - 1.3862944 * jax.random.uniform(arg_keys[2], (3, NX, NY, NZ), jnp.float32) ** shard_levels(arg_keys[2], (3, NX, NY, NZ), ((1, 4), (2, 2), (3, 4)), -0.2, 0.2)), 0.5, 2.0)
    region = place_ends(jax.random.randint(arg_keys[3], (NX, NY, NZ), 0, REGIONS), jax.random.fold_in(arg_keys[3], 1), 0, REGIONS - 1).astype(jnp.int32)
    flags = place_ends((jax.random.randint(arg_keys[4], (3, NX, NY, NZ), 0, 8) < 1).astype(jnp.int32), jax.random.fold_in(arg_keys[4], 1), 0, 1)
    return dict(rhs=rhs, conductivity=conductivity, fraction=fraction, region=region, flags=flags)


edge_damping = 0.8
node_damping = 0.8


def upward(field, spatial):
    return jnp.roll(field, -1, axis=spatial)


def downward(field, spatial):
    return jnp.roll(field, 1, axis=spatial)


def forward_diff(field, spatial):
    return upward(field, spatial) - field


def backward_adjoint(field, spatial):
    return downward(field, spatial) - field


def curl_curl(stacked):
    first, second, third = stacked[0], stacked[1], stacked[2]
    face_zero = forward_diff(third, 1) - forward_diff(second, 2)
    face_one = forward_diff(first, 2) - forward_diff(third, 0)
    face_two = forward_diff(second, 0) - forward_diff(first, 1)
    return jnp.stack([backward_adjoint(face_one, 2) - backward_adjoint(face_two, 1),
                      backward_adjoint(face_two, 0) - backward_adjoint(face_zero, 2),
                      backward_adjoint(face_zero, 1) - backward_adjoint(face_one, 0)])


def conductance(conductivity, region):
    total = jnp.zeros(region.shape, conductivity.dtype)
    for number in range(conductivity.shape[0]):
        total = total + jnp.where(region == number, conductivity[number], jnp.zeros((), conductivity.dtype))
    return total


def masked_operator(field, keeping, sigma):
    masked = keeping * field
    return keeping * (curl_curl(masked) + sigma * masked) + (1.0 - keeping) * field


def nodal_operator(stacked):
    result = 7.0 * stacked
    for spatial in range(3):
        result = result - (jnp.roll(stacked, -1, axis=spatial + 1) + jnp.roll(stacked, 1, axis=spatial + 1))
    return result


def nodal_part(masked_res):
    gradient_rhs = backward_adjoint(masked_res[0], 0)
    for spatial in range(1, 3):
        gradient_rhs = gradient_rhs + backward_adjoint(masked_res[spatial], spatial)
    vector_rhs = [(masked_res[spatial] + downward(masked_res[spatial], spatial)) * 0.5 for spatial in range(3)]
    nodal_rhs = jnp.stack([gradient_rhs] + vector_rhs)
    first_node = node_damping * nodal_rhs / 7.0
    second_node = first_node + node_damping * (nodal_rhs - nodal_operator(first_node)) / 7.0
    potential = second_node[0]
    parts = [forward_diff(potential, spatial) + (second_node[spatial + 1] + upward(second_node[spatial + 1], spatial)) * 0.5 for spatial in range(3)]
    return jnp.stack(parts)


def reference(rhs, conductivity, fraction, region, flags):
    sigma = conductance(conductivity, region)[None] * fraction
    keeping = 1.0 - flags.astype(jnp.float32)
    inverse = 1.0 / (keeping * (4.0 + sigma) + (1.0 - keeping))
    first_iter = edge_damping * inverse * rhs
    second_iter = first_iter + edge_damping * inverse * (rhs - masked_operator(first_iter, keeping, sigma))
    residual = rhs - masked_operator(second_iter, keeping, sigma)
    correction = keeping * nodal_part(keeping * residual)
    return second_iter + correction
```

```python
import functools

import jax
import jax.numpy as jnp
from jax import lax
from jax.experimental import pallas as pl
from jax.experimental.pallas import tpu as pltpu
from jax.sharding import PartitionSpec as P

damping = 0.8
c_node = 0.8 / 7.0
MESH = pl.DeviceIdType.MESH
PAD = 4
SEG = 16


def rot(v, shift, axis):
    return pltpu.roll(v, shift % v.shape[axis], axis)


def y_up(v):
    return rot(v, -1, 0)


def y_down(v):
    return rot(v, 1, 0)


def z_up(v):
    return rot(v, -1, 1)


def z_down(v):
    return rot(v, 1, 1)


def face_zero(u1, u2):
    return (y_up(u2) - u2) - (z_up(u1) - u1)


def face_one(u0, u2, u2p):
    return (z_up(u0) - u0) - (u2p - u2)


def face_two(u0, u1, u1p):
    return (u1p - u1) - (y_up(u0) - u0)


def edges(f0, f1, f2, f1m, f2m):
    return (
        (z_down(f1) - f1) - (y_down(f2) - f2),
        (f2m - f2) - (z_down(f0) - f0),
        (y_down(f0) - f0) - (f1m - f1),
    )


def jacobi_scale(ks):
    return damping / jnp.where(ks > 0.0, 4.0 + ks, 1.0)


def start_iter(rhs, ks):
    return jnp.where(ks > 0.0, jacobi_scale(ks) * rhs, 0.0)


def next_iter(rhs, ks, u, cc):
    new = u + jacobi_scale(ks) * (rhs - (cc + ks * u))
    return jnp.where(ks > 0.0, new, 0.0)


def masked_residual(rhs, ks, u, cc):
    return jnp.where(ks > 0.0, rhs - (cc + ks * u), 0.0)


def nodal_rhs(m0, m0m, m1, m2):
    m1m, m2m = y_down(m1), z_down(m2)
    return (
        (m0m - m0) + (m1m - m1) + (m2m - m2),
        (m0 + m0m) * 0.5,
        (m1 + m1m) * 0.5,
        (m2 + m2m) * 0.5,
    )


def nodal_step(r, rm, rp):
    around = (rm + rp) + (y_up(r) + y_down(r)) + (z_up(r) + z_down(r))
    return (1.2 * c_node) * r + (c_node * c_node) * around


def finish(rhs, ks, u, corr):
    fixed = damping * rhs
    fixed = fixed + damping * (rhs - fixed)
    return jnp.where(ks > 0.0, u + corr, fixed)


def kernel(
    sizes, nx, ny, nz, cond, rhs_ref, frac_ref, reg_ref, flag_ref, out_ref,
    e, w, wz, xs, xr, ys, yr, u1, u2, mm, rr, send, recv,
):
    gx, gy, gz = sizes
    ix, iy, iz = lax.axis_index("gx"), lax.axis_index("gy"), lax.axis_index("gz")
    tiles = nx * SEG // nz
    planes = nx + 2 * PAD
    per = nz // SEG

    def device(axis, step):
        pos = {"gx": ix, "gy": iy, "gz": iz}
        size = {"gx": gx, "gy": gy, "gz": gz}
        return {axis: lax.rem(pos[axis] + (step + size[axis]), size[axis])}

    partners = [device("gx", 1), device("gx", -1), device("gz", 1), device("gz", -1), device("gy", 1)]
    if gy > 2:
        partners.append(device("gy", -1))
    barrier = pltpu.get_barrier_semaphore()
    for partner in partners:
        pl.semaphore_signal(barrier, inc=1, device_id=partner, device_id_type=MESH)

    lane = lax.broadcasted_iota(jnp.int32, (ny, nz), 1)
    slot = lane // SEG

    packs = [[None] * tiles for _ in range(6)]
    for x in range(nx):
        region = reg_ref[x]
        sigma = jnp.zeros((ny, nz), jnp.float32)
        for number in range(cond.shape[0]):
            sigma = jnp.where(region == number, cond[number], sigma)
        for k in range(3):
            ks = jnp.where(flag_ref[k, x] == 0, sigma * frac_ref[k, x], 0.0)
            for f, v in ((k, rhs_ref[k, x]), (3 + k, ks)):
                e[f, PAD + x, 0:ny, :] = v
                t, j = divmod(x, per)
                piece = rot(v, 8 + SEG * j, 1)
                old = packs[f][t]
                packs[f][t] = piece if old is None else jnp.where(slot == j, piece, old)
    for f in range(6):
        for t in range(tiles):
            w[f, t] = packs[f][t]

    pl.semaphore_wait(barrier, len(partners))

    def copy(number, src, dst, where):
        made = pltpu.make_async_remote_copy(
            src_ref=src, dst_ref=dst, send_sem=send.at[number], recv_sem=recv.at[number],
            device_id=where, device_id_type=MESH,
        )
        made.start()
        return made

    z_copies = [
        copy(0, w, wz.at[0], device("gz", 1)),
        copy(1, w, wz.at[1], device("gz", -1)),
    ]
    x_copies = [
        copy(2, e.at[:, pl.ds(PAD + nx - 3, 3), pl.ds(0, ny)], e.at[:, pl.ds(1, 3), pl.ds(0, ny)], device("gx", 1)),
        copy(3, e.at[:, pl.ds(PAD, 4), pl.ds(0, ny)], e.at[:, pl.ds(PAD + nx, 4), pl.ds(0, ny)], device("gx", -1)),
    ]
    for c in z_copies:
        c.wait()
    left = (lane % SEG) < 8
    base_a = planes
    base_b = planes + tiles + 1
    half = nz // 2
    for f in range(6):
        ab = []
        for t in range(tiles):
            own = w[f, t]
            a = jnp.where(left, own, wz[1, f, t])
            b = jnp.where(left, wz[0, f, t], own)
            e[f, base_a + t, 0:ny, :] = a
            e[f, base_b + t, 0:ny, :] = b
            ab.append((a, b))
        xs[0, f] = jnp.where(lane < half, rot(ab[-1][1], half, 1), ab[-1][0])
        xs[1, f] = jnp.where(lane < half, ab[0][0], rot(ab[0][1], half, 1))
    x_copies += [
        copy(4, xs.at[0], xr.at[0], device("gx", 1)),
        copy(5, xs.at[1], xr.at[1], device("gx", -1)),
    ]
    for c in x_copies:
        c.wait()
    for f in range(6):
        minus, plus = xr[0, f], xr[1, f]
        e[f, base_a + tiles, 0:ny, :] = jnp.where(lane < half, plus, minus)
        e[f, base_b + tiles, 0:ny, :] = rot(jnp.where(lane < half, minus, plus), half, 1)

    total = planes + 2 * (tiles + 1)
    row = lax.broadcasted_iota(jnp.int32, (8, nz), 0)
    for f in range(6):
        for p in range(1, total):
            ys[f, p] = jnp.where(row < 4, e[f, p, 0:8, :], e[f, p, ny - 8:ny, :])
    if gy == 2:
        copy(6, ys, yr.at[0], device("gy", 1)).wait()
    else:
        c0 = copy(6, ys, yr.at[0], device("gy", -1))
        c1 = copy(7, ys, yr.at[1], device("gy", 1))
        c0.wait()
        c1.wait()
    for f in range(6):
        for p in range(1, total):
            tile = yr[0, f, p] if gy == 2 else jnp.where(row < 4, yr[0, f, p], yr[1, f, p])
            e[f, p, ny:ny + 8, :] = tile

    lane24 = lax.broadcasted_iota(jnp.int32, (ny + 8, nz), 1)

    def x_up(vs):
        rs = [rot(v, -SEG, 1) for v in vs]
        return [jnp.where(lane24 < nz - SEG, rs[t], rs[(t + 1) % len(rs)]) for t in range(len(rs))]

    def x_down(vs):
        rs = [rot(v, SEG, 1) for v in vs]
        return [jnp.where(lane24 >= SEG, rs[t], rs[t - 1]) for t in range(len(rs))]

    count = tiles + 1

    def strip_curl(u):
        u1p, u2p = x_up(u[1]), x_up(u[2])
        f0 = [face_zero(u[1][t], u[2][t]) for t in range(count)]
        f1 = [face_one(u[0][t], u[2][t], u2p[t]) for t in range(count)]
        f2 = [face_two(u[0][t], u[1][t], u1p[t]) for t in range(count)]
        f1m, f2m = x_down(f1), x_down(f2)
        out = [edges(f0[t], f1[t], f2[t], f1m[t], f2m[t]) for t in range(count)]
        return [[out[t][k] for t in range(count)] for k in range(3)]

    ends = []
    for base in (base_a, base_b):
        def sr(k, t):
            return e[k, base + t]

        def sk(k, t):
            return e[3 + k, base + t]

        span = range(count)
        u = [[start_iter(sr(k, t), sk(k, t)) for t in span] for k in range(3)]
        cc = strip_curl(u)
        u = [[next_iter(sr(k, t), sk(k, t), u[k][t], cc[k][t]) for t in span] for k in range(3)]
        cc = strip_curl(u)
        m = [[masked_residual(sr(k, t), sk(k, t), u[k][t], cc[k][t]) for t in span] for k in range(3)]
        m0m = x_down(m[0])
        r = [nodal_rhs(m[0][t], m0m[t], m[1][t], m[2][t]) for t in span]
        s = []
        for q in range(4):
            rq = [r[t][q] for t in span]
            rm, rp = x_down(rq), x_up(rq)
            s.append([nodal_step(rq[t], rm[t], rp[t]) for t in span])
        s0p, s1p = x_up(s[0]), x_up(s[1])
        result = []
        for t in range(tiles):
            corr = (
                (s0p[t] - s[0][t]) + (s[1][t] + s1p[t]) * 0.5,
                (y_up(s[0][t]) - s[0][t]) + (s[2][t] + y_up(s[2][t])) * 0.5,
                (z_up(s[0][t]) - s[0][t]) + (s[3][t] + z_up(s[3][t])) * 0.5,
            )
            result.append([finish(sr(k, t), sk(k, t), u[k][t], corr[k])[0:ny] for k in range(3)])
        ends.append(result)
    for t in range(tiles):
        for k in range(3):
            w[k, t] = jnp.where(left, ends[0][t][k], ends[1][t][k])

    for p in range(1, planes):
        for k in range(3):
            u1[k, p] = start_iter(e[k, p], e[3 + k, p])

    def curl_sweep(u, lo, hi, emit):
        def faces(p):
            v0, v1, v2 = u[0, p], u[1, p], u[2, p]
            return face_one(v0, v2, u[2, p + 1]), face_two(v0, v1, u[1, p + 1])

        f1m, f2m = faces(lo - 1)
        for p in range(lo, hi):
            f1, f2 = faces(p)
            f0 = face_zero(u[1, p], u[2, p])
            cc = edges(f0, f1, f2, f1m, f2m)
            for k in range(3):
                emit(k, p, cc[k])
            f1m, f2m = f1, f2

    def emit_second(k, p, cc):
        u2[k, p] = next_iter(e[k, p], e[3 + k, p], u1[k, p], cc)

    curl_sweep(u1, PAD - 2, PAD + nx + 3, emit_second)

    def emit_masked(k, p, cc):
        mm[k, p] = masked_residual(e[k, p], e[3 + k, p], u2[k, p], cc)

    curl_sweep(u2, PAD - 1, PAD + nx + 2, emit_masked)
    p = PAD - 2
    v0, v1, v2 = u2[0, p], u2[1, p], u2[2, p]
    f1 = face_one(v0, v2, u2[2, p + 1])
    f2 = face_two(v0, v1, u2[1, p + 1])
    emit_masked(0, p, (z_down(f1) - f1) - (y_down(f2) - f2))

    p = PAD + nx + 2
    for p in range(PAD - 1, PAD + nx + 2):
        r = nodal_rhs(mm[0, p], mm[0, p - 1], mm[1, p], mm[2, p])
        for q in range(4):
            rr[q, p] = r[q]

    inner = (lane >= 4) & (lane < nz - 4)
    s_next = [nodal_step(rr[q, PAD], rr[q, PAD - 1], rr[q, PAD + 1]) for q in range(4)]
    for x in range(nx):
        p = PAD + x
        s = s_next
        s_next = [nodal_step(rr[q, p + 1], rr[q, p], rr[q, p + 2]) for q in range(4)] if x < nx - 1 else [
            nodal_step(rr[q, p + 1], rr[q, p], rr[q, p + 2]) for q in range(2)
        ]
        corr = (
            (s_next[0] - s[0]) + (s[1] + s_next[1]) * 0.5,
            (y_up(s[0]) - s[0]) + (s[2] + y_up(s[2])) * 0.5,
            (z_up(s[0]) - s[0]) + (s[3] + z_up(s[3])) * 0.5,
        )
        t, j = divmod(x, per)
        for k in range(3):
            body = finish(e[k, p, 0:ny], e[3 + k, p, 0:ny], u2[k, p, 0:ny], corr[k][0:ny])
            out_ref[k, x] = jnp.where(inner, body, rot(w[k, t], nz - 8 - SEG * j, 1))


def on_device(sizes, rhs, conductivity, fraction, region, flags):
    _, nx, ny, nz = rhs.shape
    tiles = nx * SEG // nz
    planes = nx + 2 * PAD
    total = planes + 2 * (tiles + 1)
    rows = ny + 8
    f32 = jnp.float32
    vmem = pl.BlockSpec(memory_space=pltpu.VMEM)
    sides = 1 if sizes[1] == 2 else 2
    return pl.pallas_call(
        functools.partial(kernel, sizes, nx, ny, nz),
        out_shape=jax.ShapeDtypeStruct(rhs.shape, rhs.dtype),
        in_specs=[pl.BlockSpec(memory_space=pltpu.SMEM)] + [vmem] * 4,
        out_specs=vmem,
        scratch_shapes=[
            pltpu.VMEM((6, total, rows, nz), f32),
            pltpu.VMEM((6, tiles, ny, nz), f32),
            pltpu.VMEM((2, 6, tiles, ny, nz), f32),
            pltpu.VMEM((2, 6, ny, nz), f32),
            pltpu.VMEM((2, 6, ny, nz), f32),
            pltpu.VMEM((6, total, 8, nz), f32),
            pltpu.VMEM((sides, 6, total, 8, nz), f32),
            pltpu.VMEM((3, planes, rows, nz), f32),
            pltpu.VMEM((3, planes, rows, nz), f32),
            pltpu.VMEM((3, planes, rows, nz), f32),
            pltpu.VMEM((4, planes, rows, nz), f32),
            pltpu.SemaphoreType.DMA((8,)),
            pltpu.SemaphoreType.DMA((8,)),
        ],
        compiler_params=pltpu.CompilerParams(
            collective_id=0, has_side_effects=True, vmem_limit_bytes=60 * 1024 * 1024
        ),
    )(conductivity, rhs, fraction, region, flags)


def solution(mesh):
    sizes = tuple(mesh.shape[name] for name in ("gx", "gy", "gz"))
    return jax.shard_map(
        functools.partial(on_device, sizes),
        mesh=mesh,
        in_specs=(
            P(None, "gx", "gy", "gz"),
            P(),
            P(None, "gx", "gy", "gz"),
            P("gx", "gy", "gz"),
            P(None, "gx", "gy", "gz"),
        ),
        out_specs=P(None, "gx", "gy", "gz"),
        check_vma=False,
    )
```

```python
import functools

import jax
import jax.numpy as jnp
from jax import lax
from jax.experimental import pallas as pl
from jax.experimental.pallas import tpu as pltpu
from jax.sharding import PartitionSpec as P

damping = 0.8
c_node = 0.8 / 7.0
MESH = pl.DeviceIdType.MESH
PAD = 4
SEG = 16


def rot(v, shift, axis):
    return pltpu.roll(v, shift % v.shape[axis], axis)


def y_up(v):
    return rot(v, -1, 0)


def y_down(v):
    return rot(v, 1, 0)


def z_up(v):
    return rot(v, -1, 1)


def z_down(v):
    return rot(v, 1, 1)


def face_zero(u1, u2):
    return (y_up(u2) - u2) - (z_up(u1) - u1)


def face_one(u0, u2, u2p):
    return (z_up(u0) - u0) - (u2p - u2)


def face_two(u0, u1, u1p):
    return (u1p - u1) - (y_up(u0) - u0)


def edges(f0, f1, f2, f1m, f2m):
    return (
        (z_down(f1) - f1) - (y_down(f2) - f2),
        (f2m - f2) - (z_down(f0) - f0),
        (y_down(f0) - f0) - (f1m - f1),
    )


def jacobi_scale(ks):
    return damping / jnp.where(ks > 0.0, 4.0 + ks, 1.0)


def start_iter(rhs, ks):
    return jnp.where(ks > 0.0, jacobi_scale(ks) * rhs, 0.0)


def next_iter(rhs, ks, u, cc):
    new = u + jacobi_scale(ks) * (rhs - (cc + ks * u))
    return jnp.where(ks > 0.0, new, 0.0)


def masked_residual(rhs, ks, u, cc):
    return jnp.where(ks > 0.0, rhs - (cc + ks * u), 0.0)


def nodal_rhs(m0, m0m, m1, m2):
    m1m, m2m = y_down(m1), z_down(m2)
    return (
        (m0m - m0) + (m1m - m1) + (m2m - m2),
        (m0 + m0m) * 0.5,
        (m1 + m1m) * 0.5,
        (m2 + m2m) * 0.5,
    )


def nodal_step(r, rm, rp):
    around = (rm + rp) + (y_up(r) + y_down(r)) + (z_up(r) + z_down(r))
    return (1.2 * c_node) * r + (c_node * c_node) * around


def finish(rhs, ks, u, corr):
    fixed = damping * rhs
    fixed = fixed + damping * (rhs - fixed)
    return jnp.where(ks > 0.0, u + corr, fixed)


def kernel(
    sizes, nx, ny, nz, cond, rhs_hbm, frac_hbm, reg_hbm, flag_hbm, out_ref,
    rhs_ref, frac_ref, reg_ref, flag_ref,
    e, w, wz, kf, ds, dr, ya, yb, yra, yrb, u1, u2, mm, rr, load, send, recv,
):
    gx, gy, gz = sizes
    pos = {"gx": lax.axis_index("gx"), "gy": lax.axis_index("gy"), "gz": lax.axis_index("gz")}
    size = {"gx": gx, "gy": gy, "gz": gz}
    tiles = nx * SEG // nz
    planes = nx + 2 * PAD
    per = nz // SEG

    def device(**steps):
        return {axis: lax.rem(pos[axis] + (step + size[axis]), size[axis]) for axis, step in steps.items()}

    partners = [device(gx=1), device(gx=-1), device(gz=1), device(gz=-1), device(gy=1)]
    partners += [device(gx=i, gz=j) for i in (1, -1) for j in (1, -1)]
    if gy > 2:
        partners.append(device(gy=-1))
    barrier = pltpu.get_barrier_semaphore()
    for partner in partners:
        pl.semaphore_signal(barrier, inc=1, device_id=partner, device_id_type=MESH)
    loads = [
        pltpu.make_async_copy(src, dst, load.at[i])
        for i, (src, dst) in enumerate(
            ((reg_hbm, reg_ref), (frac_hbm, frac_ref), (flag_hbm, flag_ref), (rhs_hbm, rhs_ref))
        )
    ]
    for one in loads:
        one.start()
    for one in loads:
        one.wait()

    lane = lax.broadcasted_iota(jnp.int32, (ny, nz), 1)
    slot = lane // SEG
    half = nz // 2
    low_half = lane < half
    quad = (lane % SEG) // 4
    left = (lane % SEG) < 8

    def end_piece(v, j):
        return rot(v, 8 + SEG * j, 1)

    packs = [[None] * tiles for _ in range(6)]
    outer = {nx - 3: 0, 3: 1}
    sent_first = {}
    for x in range(nx):
        region = reg_ref[x]
        sigma = jnp.zeros((ny, nz), jnp.float32)
        for number in range(cond.shape[0]):
            sigma = jnp.where(region == number, cond[number], sigma)
        t, j = divmod(x, per)
        for k in range(3):
            ks = jnp.where(flag_ref[k, x] == 0, sigma * frac_ref[k, x], 0.0)
            rhs = rhs_ref[k, x]
            for f, v in ((k, rhs), (3 + k, ks)):
                e[f, PAD + x, 0:ny, :] = v
                piece = end_piece(v, j)
                old = packs[f][t]
                packs[f][t] = piece if old is None else jnp.where(slot == j, piece, old)
            if x in outer:
                first = start_iter(rhs, ks)
                kf[outer[x], k] = first
                sent_first[outer[x], k] = end_piece(first, j)
    for f in range(6):
        for t in range(tiles):
            w[f, t] = packs[f][t]
    for side in range(2):
        mine = (lane >= half) if side == 0 else low_half
        j = (nx - 3) % per if side == 0 else 3
        for zside, off in ((0, 8), (1, 4)):
            tile = None
            for f in range(6):
                v = packs[f][tiles - 1 if side == 0 else 0]
                if f < 3:
                    v = jnp.where(slot == j, sent_first[side, f], v)
                moved = rot(v, 4 * (f % 4) - off + (half if f >= 4 else 0), 1)
                where = (quad == f % 4) & (mine if f < 4 else ~mine)
                tile = moved if tile is None else jnp.where(where, moved, tile)
            ds[side, zside] = tile

    pl.semaphore_wait(barrier, len(partners))

    def copy(number, src, dst, where):
        made = pltpu.make_async_remote_copy(
            src_ref=src, dst_ref=dst, send_sem=send.at[number], recv_sem=recv.at[number],
            device_id=where, device_id_type=MESH,
        )
        made.start()
        return made

    own_rows = pl.ds(0, ny)
    z_copies = [copy(0, w, wz.at[0], device(gz=1)), copy(1, w, wz.at[1], device(gz=-1))]
    x_copies = [
        copy(2 + 2 * side + zside, ds.at[side, zside], dr.at[side, zside], device(gx=1 - 2 * side, gz=2 * zside - 1))
        for side in range(2) for zside in range(2)
    ]
    x_copies += [
        copy(6, e.at[:, pl.ds(PAD + nx - 2, 2), own_rows], e.at[:, pl.ds(2, 2), own_rows], device(gx=1)),
        copy(7, e.at[:, pl.ds(PAD, 3), own_rows], e.at[:, pl.ds(PAD + nx, 3), own_rows], device(gx=-1)),
        copy(8, kf.at[0], e.at[pl.ds(0, 3), 1, own_rows], device(gx=1)),
        copy(9, kf.at[1, pl.ds(1, 2)], e.at[pl.ds(1, 2), PAD + nx + 3, own_rows], device(gx=-1)),
    ]

    base_a = planes
    base_b = planes + tiles + 1
    row = lax.broadcasted_iota(jnp.int32, (8, nz), 0)

    def y_start(first, which, out, into):
        for f in range(6):
            for i, p in enumerate(which):
                out[f, i] = jnp.where(row < 4, e[f, p, 0:8, :], e[f, p, ny - 8:ny, :])
        if gy == 2:
            return [copy(first, out, into.at[0], device(gy=1))]
        return [
            copy(first, out, into.at[0], device(gy=-1)),
            copy(first + 1, out, into.at[1], device(gy=1)),
        ]

    def y_finish(copies, which, into):
        for one in copies:
            one.wait()
        for f in range(6):
            for i, p in enumerate(which):
                tile = into[0, f, i] if gy == 2 else jnp.where(row < 4, into[0, f, i], into[1, f, i])
                e[f, p, ny:ny + 8, :] = tile

    def curl_sweep(u, lo, hi, emit):
        def faces(p):
            v0, v1, v2 = u[0, p], u[1, p], u[2, p]
            return face_one(v0, v2, u[2, p + 1]), face_two(v0, v1, u[1, p + 1])

        f1m, f2m = faces(lo - 1)
        for p in range(lo, hi):
            f1, f2 = faces(p)
            f0 = face_zero(u[1, p], u[2, p])
            cc = edges(f0, f1, f2, f1m, f2m)
            for k in range(3):
                emit(k, p, cc[k])
            f1m, f2m = f1, f2

    def emit_second(k, p, cc):
        u2[k, p] = next_iter(e[k, p], e[3 + k, p], u1[k, p], cc)

    def emit_masked(k, p, cc):
        mm[k, p] = masked_residual(e[k, p], e[3 + k, p], u2[k, p], cc)

    def node_range(lo, hi):
        for p in range(lo, hi):
            r = nodal_rhs(mm[0, p], mm[0, p - 1], mm[1, p], mm[2, p])
            for q in range(4):
                rr[q, p] = r[q]

    def first_range(which):
        for p in which:
            for k in range(3):
                u1[k, p] = start_iter(e[k, p], e[3 + k, p])

    own = list(range(PAD, PAD + nx))
    y_own = y_start(10, own, ya, yra)
    y_finish(y_own, own, yra)
    first_range(own)
    curl_sweep(u1, PAD + 1, PAD + nx - 1, emit_second)
    curl_sweep(u2, PAD + 2, PAD + nx - 2, emit_masked)
    node_range(PAD + 3, PAD + nx - 2)

    for one in z_copies:
        one.wait()
    for f in range(6):
        for t in range(tiles):
            mid = w[f, t]
            e[f, base_a + t, 0:ny, :] = jnp.where(left, mid, wz[1, f, t])
            e[f, base_b + t, 0:ny, :] = jnp.where(left, wz[0, f, t], mid)
    for one in x_copies:
        one.wait()
    for f in range(6):
        ends = None
        for i in range(8):
            if i != 4:
                p = PAD + nx + i if i < 4 else i - 4
                piece = end_piece(e[f, p, 0:ny, :], i)
                ends = piece if ends is None else jnp.where(slot == i, piece, ends)
        corner = []
        for zside, off in ((0, 8), (1, 4)):
            plus, minus = dr[1, zside], dr[0, zside]
            if f < 4:
                corner.append(rot(jnp.where(low_half, plus, minus), off - 4 * f, 1))
            else:
                corner.append(rot(jnp.where(low_half, minus, plus), half + off - 4 * (f - 4), 1))
        e[f, base_a + tiles, 0:ny, :] = jnp.where(left, ends, corner[0])
        e[f, base_b + tiles, 0:ny, :] = jnp.where(left, corner[1], ends)
    rest = list(range(1, PAD)) + list(range(PAD + nx, planes)) + list(range(base_a, base_b + tiles + 1))
    y_rest = y_start(12, rest, yb, yrb)
    y_finish(y_rest, rest, yrb)

    lane24 = lax.broadcasted_iota(jnp.int32, (ny + 8, nz), 1)

    sent = (lane24 // SEG == 3) | (lane24 // SEG == 5)

    def x_up(vs):
        rs = [rot(v, -SEG, 1) for v in vs]
        return [jnp.where(lane24 < nz - SEG, rs[t], rs[(t + 1) % len(rs)]) for t in range(len(rs))]

    def x_down(vs):
        rs = [rot(v, SEG, 1) for v in vs]
        return [jnp.where(lane24 >= SEG, rs[t], rs[t - 1]) for t in range(len(rs))]

    count = tiles + 1

    def strip_curl(u):
        u1p, u2p = x_up(u[1]), x_up(u[2])
        f0 = [face_zero(u[1][t], u[2][t]) for t in range(count)]
        f1 = [face_one(u[0][t], u[2][t], u2p[t]) for t in range(count)]
        f2 = [face_two(u[0][t], u[1][t], u1p[t]) for t in range(count)]
        f1m, f2m = x_down(f1), x_down(f2)
        out = [edges(f0[t], f1[t], f2[t], f1m[t], f2m[t]) for t in range(count)]
        return [[out[t][k] for t in range(count)] for k in range(3)]

    ends = []
    for base in (base_a, base_b):
        def sr(k, t):
            return e[k, base + t]

        def sk(k, t):
            return e[3 + k, base + t]

        span = range(count)
        u = [[start_iter(sr(k, t), sk(k, t)) for t in span] for k in range(3)]
        for k in range(3):
            u[k][tiles] = jnp.where(sent, sr(k, tiles), u[k][tiles])
        cc = strip_curl(u)
        u = [[next_iter(sr(k, t), sk(k, t), u[k][t], cc[k][t]) for t in span] for k in range(3)]
        cc = strip_curl(u)
        m = [[masked_residual(sr(k, t), sk(k, t), u[k][t], cc[k][t]) for t in span] for k in range(3)]
        m0m = x_down(m[0])
        r = [nodal_rhs(m[0][t], m0m[t], m[1][t], m[2][t]) for t in span]
        s = []
        for q in range(4):
            rq = [r[t][q] for t in span]
            rm, rp = x_down(rq), x_up(rq)
            s.append([nodal_step(rq[t], rm[t], rp[t]) for t in span])
        s0p, s1p = x_up(s[0]), x_up(s[1])
        result = []
        for t in range(tiles):
            corr = (
                (s0p[t] - s[0][t]) + (s[1][t] + s1p[t]) * 0.5,
                (y_up(s[0][t]) - s[0][t]) + (s[2][t] + y_up(s[2][t])) * 0.5,
                (z_up(s[0][t]) - s[0][t]) + (s[3][t] + z_up(s[3][t])) * 0.5,
            )
            result.append([finish(sr(k, t), sk(k, t), u[k][t], corr[k])[0:ny] for k in range(3)])
        ends.append(result)
    for t in range(tiles):
        for k in range(3):
            w[k, t] = jnp.where(left, ends[0][t][k], ends[1][t][k])

    for k in range(3):
        u1[k, 1] = e[k, 1]
        u1[k, planes - 1] = e[k, planes - 1]
    first_range(list(range(2, PAD)) + list(range(PAD + nx, planes - 1)))
    curl_sweep(u1, PAD - 2, PAD + 1, emit_second)
    curl_sweep(u1, PAD + nx - 1, PAD + nx + 3, emit_second)
    curl_sweep(u2, PAD - 1, PAD + 2, emit_masked)
    curl_sweep(u2, PAD + nx - 2, PAD + nx + 2, emit_masked)
    p = PAD - 2
    v0, v1, v2 = u2[0, p], u2[1, p], u2[2, p]
    f1 = face_one(v0, v2, u2[2, p + 1])
    f2 = face_two(v0, v1, u2[1, p + 1])
    emit_masked(0, p, (z_down(f1) - f1) - (y_down(f2) - f2))
    node_range(PAD - 1, PAD + 3)
    node_range(PAD + nx - 2, PAD + nx + 2)

    inner = (lane >= 4) & (lane < nz - 4)
    s_next = [nodal_step(rr[q, PAD], rr[q, PAD - 1], rr[q, PAD + 1]) for q in range(4)]
    for x in range(nx):
        p = PAD + x
        s = s_next
        s_next = [nodal_step(rr[q, p + 1], rr[q, p], rr[q, p + 2]) for q in range(4)] if x < nx - 1 else [
            nodal_step(rr[q, p + 1], rr[q, p], rr[q, p + 2]) for q in range(2)
        ]
        corr = (
            (s_next[0] - s[0]) + (s[1] + s_next[1]) * 0.5,
            (y_up(s[0]) - s[0]) + (s[2] + y_up(s[2])) * 0.5,
            (z_up(s[0]) - s[0]) + (s[3] + z_up(s[3])) * 0.5,
        )
        t, j = divmod(x, per)
        for k in range(3):
            body = finish(e[k, p, 0:ny], e[3 + k, p, 0:ny], u2[k, p, 0:ny], corr[k][0:ny])
            out_ref[k, x] = jnp.where(inner, body, rot(w[k, t], nz - 8 - SEG * j, 1))


def on_device(sizes, rhs, conductivity, fraction, region, flags):
    _, nx, ny, nz = rhs.shape
    tiles = nx * SEG // nz
    planes = nx + 2 * PAD
    total = planes + 2 * (tiles + 1)
    rest = 2 * PAD - 1 + 2 * (tiles + 1)
    rows = ny + 8
    f32 = jnp.float32
    hbm = pl.BlockSpec(memory_space=pl.ANY)
    sides = 1 if sizes[1] == 2 else 2
    return pl.pallas_call(
        functools.partial(kernel, sizes, nx, ny, nz),
        out_shape=pltpu.VMEM(rhs.shape, rhs.dtype),
        in_specs=[pl.BlockSpec(memory_space=pltpu.SMEM)] + [hbm] * 4,
        out_specs=pl.BlockSpec(memory_space=pltpu.VMEM),
        scratch_shapes=[
            pltpu.VMEM(rhs.shape, f32),
            pltpu.VMEM(rhs.shape, f32),
            pltpu.VMEM(region.shape, jnp.int32),
            pltpu.VMEM(flags.shape, jnp.int32),
            pltpu.VMEM((6, total, rows, nz), f32),
            pltpu.VMEM((6, tiles, ny, nz), f32),
            pltpu.VMEM((2, 6, tiles, ny, nz), f32),
            pltpu.VMEM((2, 3, ny, nz), f32),
            pltpu.VMEM((2, 2, ny, nz), f32),
            pltpu.VMEM((2, 2, ny, nz), f32),
            pltpu.VMEM((6, nx, 8, nz), f32),
            pltpu.VMEM((6, rest, 8, nz), f32),
            pltpu.VMEM((sides, 6, nx, 8, nz), f32),
            pltpu.VMEM((sides, 6, rest, 8, nz), f32),
            pltpu.VMEM((3, planes, rows, nz), f32),
            pltpu.VMEM((3, planes, rows, nz), f32),
            pltpu.VMEM((3, planes, rows, nz), f32),
            pltpu.VMEM((4, planes, rows, nz), f32),
            pltpu.SemaphoreType.DMA((4,)),
            pltpu.SemaphoreType.DMA((14,)),
            pltpu.SemaphoreType.DMA((14,)),
        ],
        compiler_params=pltpu.CompilerParams(
            collective_id=0, has_side_effects=True, vmem_limit_bytes=40 * 1024 * 1024
        ),
    )(conductivity, rhs, fraction, region, flags)


def solution(mesh):
    sizes = tuple(mesh.shape[name] for name in ("gx", "gy", "gz"))
    return jax.shard_map(
        functools.partial(on_device, sizes),
        mesh=mesh,
        in_specs=(
            P(None, "gx", "gy", "gz"),
            P(),
            P(None, "gx", "gy", "gz"),
            P("gx", "gy", "gz"),
            P(None, "gx", "gy", "gz"),
        ),
        out_specs=P(None, "gx", "gy", "gz"),
        check_vma=False,
    )
```

```python
import functools

import jax
import jax.numpy as jnp
from jax import lax
from jax.experimental import pallas as pl
from jax.experimental.pallas import tpu as pltpu
from jax.sharding import PartitionSpec as P

damping = 0.8
c_node = 0.8 / 7.0
MESH = pl.DeviceIdType.MESH
PAD = 4
SEG = 16


def rot(v, shift, axis):
    return pltpu.roll(v, shift % v.shape[axis], axis)


def y_up(v):
    return rot(v, -1, 0)


def y_down(v):
    return rot(v, 1, 0)


def z_up(v):
    return rot(v, -1, 1)


def z_down(v):
    return rot(v, 1, 1)


def face_zero(u1, u2):
    return (y_up(u2) - u2) - (z_up(u1) - u1)


def face_one(u0, u2, u2p):
    return (z_up(u0) - u0) - (u2p - u2)


def face_two(u0, u1, u1p):
    return (u1p - u1) - (y_up(u0) - u0)


def edges(f0, f1, f2, f1m, f2m):
    return (
        (z_down(f1) - f1) - (y_down(f2) - f2),
        (f2m - f2) - (z_down(f0) - f0),
        (y_down(f0) - f0) - (f1m - f1),
    )


def jacobi_scale(ks):
    return damping / jnp.where(ks > 0.0, 4.0 + ks, 1.0)


def start_iter(rhs, ks):
    return jnp.where(ks > 0.0, jacobi_scale(ks) * rhs, 0.0)


def next_iter(rhs, ks, u, cc):
    new = u + jacobi_scale(ks) * (rhs - (cc + ks * u))
    return jnp.where(ks > 0.0, new, 0.0)


def masked_residual(rhs, ks, u, cc):
    return jnp.where(ks > 0.0, rhs - (cc + ks * u), 0.0)


def nodal_rhs(m0, m0m, m1, m2):
    m1m, m2m = y_down(m1), z_down(m2)
    return (
        (m0m - m0) + (m1m - m1) + (m2m - m2),
        (m0 + m0m) * 0.5,
        (m1 + m1m) * 0.5,
        (m2 + m2m) * 0.5,
    )


def nodal_step(r, rm, rp):
    around = (rm + rp) + (y_up(r) + y_down(r)) + (z_up(r) + z_down(r))
    return (1.2 * c_node) * r + (c_node * c_node) * around


def finish(rhs, ks, u, corr):
    fixed = damping * rhs
    fixed = fixed + damping * (rhs - fixed)
    return jnp.where(ks > 0.0, u + corr, fixed)


def kernel(
    sizes, nx, ny, nz, cond, rhs_hbm, frac_hbm, reg_hbm, flag_hbm, out_ref,
    rhs_ref, frac_ref, reg_ref, flag_ref,
    e, w, wz, kf, ds, dr, ya, yb, yra, yrb, u1, u2, mm, rr, load, send, recv,
):
    gx, gy, gz = sizes
    pos = {"gx": lax.axis_index("gx"), "gy": lax.axis_index("gy"), "gz": lax.axis_index("gz")}
    size = {"gx": gx, "gy": gy, "gz": gz}
    tiles = nx * SEG // nz
    planes = nx + 2 * PAD
    per = nz // SEG

    def device(**steps):
        return {axis: lax.rem(pos[axis] + (step + size[axis]), size[axis]) for axis, step in steps.items()}

    partners = [device(gx=1), device(gx=-1), device(gz=1), device(gz=-1), device(gy=1)]
    if gy > 2:
        partners.append(device(gy=-1))
    barrier = pltpu.get_barrier_semaphore()
    for partner in partners:
        pl.semaphore_signal(barrier, inc=1, device_id=partner, device_id_type=MESH)
    loads = [
        pltpu.make_async_copy(src, dst, load.at[i])
        for i, (src, dst) in enumerate(
            ((reg_hbm, reg_ref), (frac_hbm, frac_ref), (flag_hbm, flag_ref), (rhs_hbm, rhs_ref))
        )
    ]
    for one in loads:
        one.start()
    for one in loads:
        one.wait()

    lane = lax.broadcasted_iota(jnp.int32, (ny, nz), 1)
    slot = lane // SEG
    half = nz // 2
    low_half = lane < half
    quad = (lane % SEG) // 4
    left = (lane % SEG) < 8

    def end_piece(v, j):
        return rot(v, 8 + SEG * j, 1)

    packs = [[None] * tiles for _ in range(6)]
    outer = {nx - 3: 0, 3: 1}
    for x in range(nx):
        region = reg_ref[x]
        sigma = jnp.zeros((ny, nz), jnp.float32)
        for number in range(cond.shape[0]):
            sigma = jnp.where(region == number, cond[number], sigma)
        t, j = divmod(x, per)
        for k in range(3):
            ks = jnp.where(flag_ref[k, x] == 0, sigma * frac_ref[k, x], 0.0)
            rhs = rhs_ref[k, x]
            for f, v in ((k, rhs), (3 + k, ks)):
                e[f, PAD + x, 0:ny, :] = v
                piece = end_piece(v, j)
                old = packs[f][t]
                packs[f][t] = piece if old is None else jnp.where(slot == j, piece, old)
            if x in outer:
                kf[outer[x], k] = start_iter(rhs, ks)
    for f in range(6):
        for t in range(tiles):
            w[f, t] = packs[f][t]
    pl.semaphore_wait(barrier, len(partners))

    def copy(number, src, dst, where):
        made = pltpu.make_async_remote_copy(
            src_ref=src, dst_ref=dst, send_sem=send.at[number], recv_sem=recv.at[number],
            device_id=where, device_id_type=MESH,
        )
        made.start()
        return made

    own_rows = pl.ds(0, ny)
    z_copies = [copy(0, w, wz.at[0], device(gz=1)), copy(1, w, wz.at[1], device(gz=-1))]
    x_copies = [
        copy(6, e.at[:, pl.ds(PAD + nx - 2, 2), own_rows], e.at[:, pl.ds(2, 2), own_rows], device(gx=1)),
        copy(7, e.at[:, pl.ds(PAD, 3), own_rows], e.at[:, pl.ds(PAD + nx, 3), own_rows], device(gx=-1)),
        copy(8, kf.at[0], e.at[pl.ds(0, 3), 1, own_rows], device(gx=1)),
        copy(9, kf.at[1, pl.ds(1, 2)], e.at[pl.ds(1, 2), PAD + nx + 3, own_rows], device(gx=-1)),
    ]

    base_a = planes
    base_b = planes + tiles + 1
    row = lax.broadcasted_iota(jnp.int32, (8, nz), 0)

    def y_start(first, which, out, into):
        for f in range(6):
            for i, p in enumerate(which):
                out[f, i] = jnp.where(row < 4, e[f, p, 0:8, :], e[f, p, ny - 8:ny, :])
        if gy == 2:
            return [copy(first, out, into.at[0], device(gy=1))]
        return [
            copy(first, out, into.at[0], device(gy=-1)),
            copy(first + 1, out, into.at[1], device(gy=1)),
        ]

    def y_finish(copies, which, into):
        for one in copies:
            one.wait()
        for f in range(6):
            for i, p in enumerate(which):
                tile = into[0, f, i] if gy == 2 else jnp.where(row < 4, into[0, f, i], into[1, f, i])
                e[f, p, ny:ny + 8, :] = tile

    def curl_sweep(u, lo, hi, emit):
        def faces(p):
            v0, v1, v2 = u[0, p], u[1, p], u[2, p]
            return face_one(v0, v2, u[2, p + 1]), face_two(v0, v1, u[1, p + 1])

        f1m, f2m = faces(lo - 1)
        for p in range(lo, hi):
            f1, f2 = faces(p)
            f0 = face_zero(u[1, p], u[2, p])
            cc = edges(f0, f1, f2, f1m, f2m)
            for k in range(3):
                emit(k, p, cc[k])
            f1m, f2m = f1, f2

    def emit_second(k, p, cc):
        u2[k, p] = next_iter(e[k, p], e[3 + k, p], u1[k, p], cc)

    def emit_masked(k, p, cc):
        mm[k, p] = masked_residual(e[k, p], e[3 + k, p], u2[k, p], cc)

    def node_range(lo, hi):
        for p in range(lo, hi):
            r = nodal_rhs(mm[0, p], mm[0, p - 1], mm[1, p], mm[2, p])
            for q in range(4):
                rr[q, p] = r[q]

    def first_range(which):
        for p in which:
            for k in range(3):
                u1[k, p] = start_iter(e[k, p], e[3 + k, p])

    own = list(range(PAD, PAD + nx))
    y_own = y_start(10, own, ya, yra)
    y_finish(y_own, own, yra)
    first_range(own)
    for one in z_copies:
        one.wait()
    for side in range(2):
        mine = (lane >= half) if side == 0 else low_half
        j = (nx - 3) % per if side == 0 else 3
        t = tiles - 1 if side == 0 else 0
        for zside, off in ((0, 8), (1, 4)):
            tile = None
            for f in range(6):
                v = wz[1 - zside, f, t]
                if f < 3:
                    v = jnp.where(slot == j, start_iter(v, wz[1 - zside, 3 + f, t]), v)
                moved = rot(v, 4 * (f % 4) - off + (half if f >= 4 else 0), 1)
                where = (quad == f % 4) & (mine if f < 4 else ~mine)
                tile = moved if tile is None else jnp.where(where, moved, tile)
            ds[side, zside] = tile
    x_copies += [copy(2 + side, ds.at[side], dr.at[side], device(gx=1 - 2 * side)) for side in range(2)]
    for f in range(6):
        for t in range(tiles):
            mid = w[f, t]
            e[f, base_a + t, 0:ny, :] = jnp.where(left, mid, wz[1, f, t])
            e[f, base_b + t, 0:ny, :] = jnp.where(left, wz[0, f, t], mid)
    curl_sweep(u1, PAD + 1, PAD + nx - 1, emit_second)
    curl_sweep(u2, PAD + 2, PAD + nx - 2, emit_masked)
    node_range(PAD + 3, PAD + nx - 2)

    for one in x_copies:
        one.wait()
    for f in range(6):
        ends = None
        for i in range(8):
            if i != 4:
                p = PAD + nx + i if i < 4 else i - 4
                piece = end_piece(e[f, p, 0:ny, :], i)
                ends = piece if ends is None else jnp.where(slot == i, piece, ends)
        corner = []
        for zside, off in ((0, 8), (1, 4)):
            plus, minus = dr[1, zside], dr[0, zside]
            if f < 4:
                corner.append(rot(jnp.where(low_half, plus, minus), off - 4 * f, 1))
            else:
                corner.append(rot(jnp.where(low_half, minus, plus), half + off - 4 * (f - 4), 1))
        e[f, base_a + tiles, 0:ny, :] = jnp.where(left, ends, corner[0])
        e[f, base_b + tiles, 0:ny, :] = jnp.where(left, corner[1], ends)
    rest = list(range(1, PAD)) + list(range(PAD + nx, planes)) + list(range(base_a, base_b + tiles + 1))
    y_rest = y_start(12, rest, yb, yrb)
    y_finish(y_rest, rest, yrb)

    lane24 = lax.broadcasted_iota(jnp.int32, (ny + 8, nz), 1)

    sent = (lane24 // SEG == 3) | (lane24 // SEG == 5)

    def x_up(vs):
        rs = [rot(v, -SEG, 1) for v in vs]
        return [jnp.where(lane24 < nz - SEG, rs[t], rs[(t + 1) % len(rs)]) for t in range(len(rs))]

    def x_down(vs):
        rs = [rot(v, SEG, 1) for v in vs]
        return [jnp.where(lane24 >= SEG, rs[t], rs[t - 1]) for t in range(len(rs))]

    count = tiles + 1

    def strip_curl(u):
        u1p, u2p = x_up(u[1]), x_up(u[2])
        f0 = [face_zero(u[1][t], u[2][t]) for t in range(count)]
        f1 = [face_one(u[0][t], u[2][t], u2p[t]) for t in range(count)]
        f2 = [face_two(u[0][t], u[1][t], u1p[t]) for t in range(count)]
        f1m, f2m = x_down(f1), x_down(f2)
        out = [edges(f0[t], f1[t], f2[t], f1m[t], f2m[t]) for t in range(count)]
        return [[out[t][k] for t in range(count)] for k in range(3)]

    ends = []
    for base in (base_a, base_b):
        def sr(k, t):
            return e[k, base + t]

        def sk(k, t):
            return e[3 + k, base + t]

        span = range(count)
        u = [[start_iter(sr(k, t), sk(k, t)) for t in span] for k in range(3)]
        for k in range(3):
            u[k][tiles] = jnp.where(sent, sr(k, tiles), u[k][tiles])
        cc = strip_curl(u)
        u = [[next_iter(sr(k, t), sk(k, t), u[k][t], cc[k][t]) for t in span] for k in range(3)]
        cc = strip_curl(u)
        m = [[masked_residual(sr(k, t), sk(k, t), u[k][t], cc[k][t]) for t in span] for k in range(3)]
        m0m = x_down(m[0])
        r = [nodal_rhs(m[0][t], m0m[t], m[1][t], m[2][t]) for t in span]
        s = []
        for q in range(4):
            rq = [r[t][q] for t in span]
            rm, rp = x_down(rq), x_up(rq)
            s.append([nodal_step(rq[t], rm[t], rp[t]) for t in span])
        s0p, s1p = x_up(s[0]), x_up(s[1])
        result = []
        for t in range(tiles):
            corr = (
                (s0p[t] - s[0][t]) + (s[1][t] + s1p[t]) * 0.5,
                (y_up(s[0][t]) - s[0][t]) + (s[2][t] + y_up(s[2][t])) * 0.5,
                (z_up(s[0][t]) - s[0][t]) + (s[3][t] + z_up(s[3][t])) * 0.5,
            )
            result.append([finish(sr(k, t), sk(k, t), u[k][t], corr[k])[0:ny] for k in range(3)])
        ends.append(result)
    for t in range(tiles):
        for k in range(3):
            w[k, t] = jnp.where(left, ends[0][t][k], ends[1][t][k])

    for k in range(3):
        u1[k, 1] = e[k, 1]
        u1[k, planes - 1] = e[k, planes - 1]
    first_range(list(range(2, PAD)) + list(range(PAD + nx, planes - 1)))
    curl_sweep(u1, PAD - 2, PAD + 1, emit_second)
    curl_sweep(u1, PAD + nx - 1, PAD + nx + 3, emit_second)
    curl_sweep(u2, PAD - 1, PAD + 2, emit_masked)
    curl_sweep(u2, PAD + nx - 2, PAD + nx + 2, emit_masked)
    p = PAD - 2
    v0, v1, v2 = u2[0, p], u2[1, p], u2[2, p]
    f1 = face_one(v0, v2, u2[2, p + 1])
    f2 = face_two(v0, v1, u2[1, p + 1])
    emit_masked(0, p, (z_down(f1) - f1) - (y_down(f2) - f2))
    node_range(PAD - 1, PAD + 3)
    node_range(PAD + nx - 2, PAD + nx + 2)

    inner = (lane >= 4) & (lane < nz - 4)
    s_next = [nodal_step(rr[q, PAD], rr[q, PAD - 1], rr[q, PAD + 1]) for q in range(4)]
    for x in range(nx):
        p = PAD + x
        s = s_next
        s_next = [nodal_step(rr[q, p + 1], rr[q, p], rr[q, p + 2]) for q in range(4)] if x < nx - 1 else [
            nodal_step(rr[q, p + 1], rr[q, p], rr[q, p + 2]) for q in range(2)
        ]
        corr = (
            (s_next[0] - s[0]) + (s[1] + s_next[1]) * 0.5,
            (y_up(s[0]) - s[0]) + (s[2] + y_up(s[2])) * 0.5,
            (z_up(s[0]) - s[0]) + (s[3] + z_up(s[3])) * 0.5,
        )
        t, j = divmod(x, per)
        for k in range(3):
            body = finish(e[k, p, 0:ny], e[3 + k, p, 0:ny], u2[k, p, 0:ny], corr[k][0:ny])
            out_ref[k, x] = jnp.where(inner, body, rot(w[k, t], nz - 8 - SEG * j, 1))


def on_device(sizes, rhs, conductivity, fraction, region, flags):
    _, nx, ny, nz = rhs.shape
    tiles = nx * SEG // nz
    planes = nx + 2 * PAD
    total = planes + 2 * (tiles + 1)
    rest = 2 * PAD - 1 + 2 * (tiles + 1)
    rows = ny + 8
    f32 = jnp.float32
    hbm = pl.BlockSpec(memory_space=pl.ANY)
    sides = 1 if sizes[1] == 2 else 2
    return pl.pallas_call(
        functools.partial(kernel, sizes, nx, ny, nz),
        out_shape=pltpu.VMEM(rhs.shape, rhs.dtype),
        in_specs=[pl.BlockSpec(memory_space=pltpu.SMEM)] + [hbm] * 4,
        out_specs=pl.BlockSpec(memory_space=pltpu.VMEM),
        scratch_shapes=[
            pltpu.VMEM(rhs.shape, f32),
            pltpu.VMEM(rhs.shape, f32),
            pltpu.VMEM(region.shape, jnp.int32),
            pltpu.VMEM(flags.shape, jnp.int32),
            pltpu.VMEM((6, total, rows, nz), f32),
            pltpu.VMEM((6, tiles, ny, nz), f32),
            pltpu.VMEM((2, 6, tiles, ny, nz), f32),
            pltpu.VMEM((2, 3, ny, nz), f32),
            pltpu.VMEM((2, 2, ny, nz), f32),
            pltpu.VMEM((2, 2, ny, nz), f32),
            pltpu.VMEM((6, nx, 8, nz), f32),
            pltpu.VMEM((6, rest, 8, nz), f32),
            pltpu.VMEM((sides, 6, nx, 8, nz), f32),
            pltpu.VMEM((sides, 6, rest, 8, nz), f32),
            pltpu.VMEM((3, planes, rows, nz), f32),
            pltpu.VMEM((3, planes, rows, nz), f32),
            pltpu.VMEM((3, planes, rows, nz), f32),
            pltpu.VMEM((4, planes, rows, nz), f32),
            pltpu.SemaphoreType.DMA((4,)),
            pltpu.SemaphoreType.DMA((14,)),
            pltpu.SemaphoreType.DMA((14,)),
        ],
        compiler_params=pltpu.CompilerParams(
            collective_id=0, has_side_effects=True, vmem_limit_bytes=60 * 1024 * 1024
        ),
    )(conductivity, rhs, fraction, region, flags)


def solution(mesh):
    sizes = tuple(mesh.shape[name] for name in ("gx", "gy", "gz"))
    return jax.shard_map(
        functools.partial(on_device, sizes),
        mesh=mesh,
        in_specs=(
            P(None, "gx", "gy", "gz"),
            P(),
            P(None, "gx", "gy", "gz"),
            P("gx", "gy", "gz"),
            P(None, "gx", "gy", "gz"),
        ),
        out_specs=P(None, "gx", "gy", "gz"),
        check_vma=False,
    )
```
